32 devices in a mesh: groups: 2 (over x), dev: 4 (over y, core), tp: 4 (over z).
Axes of the slice: x: 2, y: 2, z: 4, core: 2. Of those that a mesh axis runs over, the one named last changes fastest.
Arguments:
- hidden_states: bfloat16 [5120, 5120], P(('groups', 'dev'), 'tp'), parts along dimension 0, may hold values from -6 to 6
- norm_gain: bfloat16 [5120], replicated, may hold values from 0.25 to 1.75
- w_query: bfloat16 [5120, 5120], P('dev', 'tp'), may hold values from -2 to 2
- w_key: bfloat16 [5120, 1024], P('dev', 'tp'), may hold values from -2 to 2
- w_value: bfloat16 [5120, 1024], P('dev', 'tp'), may hold values from -0.078125 to 0.078125
- prompt_blocks: int32 [16], P('groups'), parts along dimension 0, may hold values from 1 to 3, 20 in all
- owner_map: int32 [40], P(('groups', 'dev')), parts along dimension 0, may hold values from 0 to 3, as said below
- slot_table: int32 [8, 8], P(('groups', 'dev')), parts along dimension 0, may hold values from 0 to 7, each once within a row
Outputs:
- context: bfloat16 [5120, 5120], P(('groups', 'dev'), 'tp'), parts along dimension 0
- kv_cache: bfloat16 [64, 128, 2048], P(('groups', 'dev'), None, 'tp'), parts along dimension 0
The draws below stay inside these ranges and needn't reach their ends.
There are 2 independent parts, one for each index of `groups`. The reference program is written for one: setup_inputs(seed, part) draws one part's arguments, and reference() takes and returns one part's arrays. A program takes and returns all parts, laid end to end along the dimension named above; an argument that names none is the same for every part. Nothing has to cross between parts.
Inputs may be any that keep to these rules, and one draw needn't show every extreme that they name: `prompt_blocks`: the entries sum to 20. `owner_map`: each device's 5 blocks name any owner at most 2 times, and no owner receives more than 8 blocks; in every draw some owner receives 2 blocks from every device. `slot_table`: each row is a permutation of 0 to 7.
All inputs are finite; a program needn't handle non-finite values.
Results may differ from the reference program's by a relative error of at most 0.0079.
Values may be sent and summed in bfloat16 or wider, within the bound.
A program may use at most 128 MiB of HBM per device.

```python
import math
import jax
import jax.numpy as jnp
import numpy as np
from jax import lax

D = 5120
HD = 128
KV_HEADS = 8
HEADS = 40
BLOCK = 128
PROMPTS = 8
PAIR_CAP = 2
TOKENS = 2560
BLK_DEV = 5
BLOCKS = 20
LEN_BLOCKS = 3
SLOTS = 8
N_DEV = 4


def joint_weights(key):
    base = jax.random.fold_in(key, 7171)
    factor = D ** (-0.5)
    group_size = HEADS // KV_HEADS
    key_part = jax.random.truncated_normal(jax.random.fold_in(base, 1), -4.0, 4.0, (D, KV_HEADS, HD), jnp.float32) * factor
    query_part = jax.random.truncated_normal(jax.random.fold_in(base, 4), -4.0, 4.0, (D, KV_HEADS, group_size, HD), jnp.float32) * factor
    return (query_part.reshape(D, HEADS * HD), key_part.reshape(D, KV_HEADS * HD))


def draw_w_query(key, part):
    return joint_weights(key)[0].astype(jnp.bfloat16)


def draw_w_key(key, part):
    return joint_weights(key)[1].astype(jnp.bfloat16)


def draw_owner_map(key, part):
    hottest = jax.random.randint(jax.random.fold_in(key, 5), (), 0, N_DEV)

    def one_device(device):
        stream = jax.random.fold_in(key, 100 + device)
        first_pass = jax.random.permutation(jax.random.fold_in(stream, 1), N_DEV - 1)
        second_pass = jax.random.permutation(jax.random.fold_in(stream, 2), N_DEV - 1)
        others = jnp.concatenate([first_pass, second_pass])[:BLK_DEV - PAIR_CAP]
        others = others + (others >= hottest).astype(jnp.int32)
        picks = jnp.concatenate([jnp.full((PAIR_CAP,), hottest, jnp.int32), others.astype(jnp.int32)])
        shuffle = jax.random.permutation(jax.random.fold_in(stream, 3), BLK_DEV)
        return picks[shuffle]
    return jax.vmap(one_device)(jnp.arange(N_DEV, dtype=jnp.int32)).reshape(-1).astype(jnp.int32)


def shard_levels(stream_key, dims, cuts, low, largest):
    loudness, own = 1.0, jax.random.fold_in(stream_key, 6)
    for axis_at, shards_of in cuts:
        draws = jnp.exp(jax.random.uniform(jax.random.fold_in(own, axis_at), (shards_of,), jnp.float32, low / len(cuts), largest / len(cuts)))
        loudness = loudness * jnp.repeat(draws, dims[axis_at] // shards_of).reshape([-1 if axis == axis_at else 1 for axis in range(len(dims))])
    return loudness


def length_profile(count, total, limit, lean):
    weights = [(1 << 20) // math.isqrt(standing ** lean) + 1 for standing in range(2, count + 1)]
    surplus, counts = total - limit - (count - 1), [1] * (count - 1)
    while surplus > 0:
        free = [i for i in range(count - 1) if counts[i] < limit]
        mass, budget = sum([weights[i] for i in free]), surplus
        for i in free:
            extra = min(limit - counts[i], max(1, budget * weights[i] // mass), surplus)
            counts[i] = counts[i] + extra
            surplus = surplus - extra
    return np.array([limit] + counts)


def uneven(stream_key, amount, total, most, lean):
    if amount == 2:
        one = jax.random.randint(stream_key, (), max(1, total - most), min(most, total - 1) + 1)
        return jnp.stack([one, total - one])
    sizes = jnp.asarray(length_profile(amount, total, most, lean), jnp.int32)
    twos = (amount - 1) // 2
    donor, taker = sizes[1:1 + 2 * twos:2], sizes[2:2 + 2 * twos:2]
    room = jnp.minimum(donor - 1, most - taker)
    moved = jax.random.randint(jax.random.fold_in(stream_key, 1), (twos,), 0, 1 << 20) % (room + 1)
    sizes = sizes.at[1:1 + 2 * twos:2].set(donor - moved).at[2:2 + 2 * twos:2].set(taker + moved)
    return sizes[jax.random.permutation(jax.random.fold_in(stream_key, 2), amount)]


def bell_draw(key, shape, deviation, limit, cuts=(), kind=jnp.bfloat16):
    values = deviation * jax.random.normal(key, shape, jnp.float32)
    if cuts:
        values = values * shard_levels(key, shape, cuts, -0.22, 0.18)
    return jnp.clip(values, -limit, limit).astype(kind)


def setup_inputs(seed: int = 0, part: int = 0) -> dict:
    seeds = jax.random.split(jax.random.key(seed), 9)
    part_splits = jax.random.split(jax.random.fold_in(seeds[8], part), 9)
    hidden_states = bell_draw(part_splits[0], (TOKENS, D), 1.0, 6.0, ((0, 4), (1, 4)))
    norm_gain = jnp.clip(1.0 + 0.15 * jax.random.normal(seeds[1], (D,), jnp.float32), 0.25, 1.75).astype(jnp.bfloat16)
    w_query = draw_w_query(jax.random.fold_in(seeds[8], 71), part)
    w_key = draw_w_key(jax.random.fold_in(seeds[8], 71), part)
    w_value = bell_draw(seeds[4], (D, KV_HEADS * HD), D ** -0.5, 0.078125, ((0, 4), (1, 4)))
    prompt_blocks = uneven(part_splits[5], PROMPTS, BLOCKS, LEN_BLOCKS, 2).astype(jnp.int32)
    owner_map = draw_owner_map(jax.random.fold_in(jax.random.fold_in(seeds[8], part), 71), part)
    slot_table = jax.vmap(lambda own: jax.random.permutation(own, SLOTS))(jax.random.split(part_splits[7], N_DEV)).reshape((N_DEV, SLOTS)).astype(jnp.int32)
    return {"hidden_states": hidden_states, "norm_gain": norm_gain, "w_query": w_query, "w_key": w_key, "w_value": w_value, "prompt_blocks": prompt_blocks, "owner_map": owner_map, "slot_table": slot_table}


EPSILON = 1e-06
THETA = 1000000.0

def prompt_start(positions, starts):
    return lax.optimization_barrier(jnp.max(jnp.where(positions[:, None] >= starts[None, :], starts[None, :], 0), axis=1))

def rotate(heads, offsets):
    half_width = heads.shape[-1] // 2
    freq_index = jnp.arange(half_width, dtype=jnp.float32)
    inverse = jnp.exp(freq_index * (-2.0 * math.log(THETA) / heads.shape[-1]))
    angles = offsets.astype(jnp.float32)[:, None] * inverse[None, :]
    cosine = jnp.cos(angles)[:, None, :]
    sine_part = jnp.sin(angles)[:, None, :]
    first_half = heads[..., :half_width]
    second = heads[..., half_width:]
    return jnp.concatenate([first_half * cosine - second * sine_part, second * cosine + first_half * sine_part], axis=-1)

def reference(hidden_states, norm_gain, w_query, w_key, w_value, prompt_blocks, owner_map, slot_table):
    floats = hidden_states.astype(jnp.float32)
    square = lax.optimization_barrier(jnp.mean(floats * floats, axis=1, keepdims=True))
    normed = (floats * lax.rsqrt(square + EPSILON) * norm_gain.astype(jnp.float32)).astype(jnp.bfloat16)
    query_proj = jnp.dot(normed, w_query, preferred_element_type=jnp.float32)
    key_proj = jnp.dot(normed, w_key, preferred_element_type=jnp.float32)
    value_proj = jnp.dot(normed, w_value, preferred_element_type=jnp.float32)
    group_size = HEADS // KV_HEADS
    token_rows = jnp.arange(TOKENS, dtype=jnp.int32)
    starts = ((jnp.cumsum(prompt_blocks) - prompt_blocks) * BLOCK).astype(jnp.int32)
    start_of = prompt_start(token_rows, starts)
    offsets = token_rows - start_of
    queries = rotate(query_proj.reshape(TOKENS, HEADS, HD), offsets).astype(jnp.bfloat16)
    rope_keys = rotate(key_proj.reshape(TOKENS, KV_HEADS, HD), offsets).astype(jnp.bfloat16)
    values = value_proj.reshape(TOKENS, KV_HEADS, HD).astype(jnp.bfloat16)
    window = LEN_BLOCKS * BLOCK + BLOCK
    score_scale = 1.0 / math.sqrt(HD)

    def one_block(block_index):
        first_row = (block_index * BLOCK).astype(jnp.int32)
        window_start = jnp.maximum(first_row + BLOCK - window, 0).astype(jnp.int32)
        block_queries = lax.dynamic_slice_in_dim(queries, first_row, BLOCK, 0).astype(jnp.float32)
        block_queries = block_queries.reshape(BLOCK, KV_HEADS, group_size, HD)
        block_keys = lax.dynamic_slice_in_dim(rope_keys, window_start, window, 0).astype(jnp.float32)
        block_values = lax.dynamic_slice_in_dim(values, window_start, window, 0).astype(jnp.float32)
        query_rows = first_row + jnp.arange(BLOCK, dtype=jnp.int32)
        key_rows = window_start + jnp.arange(window, dtype=jnp.int32)
        query_start = lax.dynamic_slice_in_dim(start_of, first_row, BLOCK, 0)
        key_start = lax.dynamic_slice_in_dim(start_of, window_start, window, 0)
        allowed = (query_start[:, None] == key_start[None, :]) & (key_rows[None, :] <= query_rows[:, None])
        allowed_heads = allowed[:, None, None, :]
        scores = jnp.einsum('tkgd,wkd->tkgw', block_queries, block_keys) * score_scale
        scores = jnp.where(allowed_heads, scores, -1e+30)
        row_max = lax.optimization_barrier(jnp.max(scores, axis=-1, keepdims=True))
        weights = jnp.where(allowed_heads, jnp.exp(scores - row_max), 0.0)
        row_total = lax.optimization_barrier(jnp.sum(weights, axis=-1))
        rounded = lax.optimization_barrier(weights.astype(jnp.bfloat16)).astype(jnp.float32)
        weighted = jnp.einsum('tkgw,wkd->tkgd', rounded, block_values)
        return (weighted / row_total[..., None]).reshape(BLOCK, HEADS * HD).astype(jnp.bfloat16)
    context = lax.map(one_block, jnp.arange(TOKENS // BLOCK, dtype=jnp.int32)).reshape(TOKENS, HEADS * HD)
    owner_hits = (owner_map[:, None] == jnp.arange(N_DEV, dtype=jnp.int32)[None, :]).astype(jnp.int32)
    earlier_hits = jnp.cumsum(owner_hits, axis=0) - owner_hits
    ranks = lax.optimization_barrier(jnp.sum(earlier_hits * owner_hits, axis=1)).astype(jnp.int32)
    slots = slot_table[owner_map, ranks]
    target = (owner_map * SLOTS + slots).astype(jnp.int32)
    packed = jnp.stack([rope_keys, values], axis=2).reshape(BLOCKS, BLOCK, 2 * KV_HEADS * HD)
    kv_cache = jnp.zeros((N_DEV * SLOTS, BLOCK, 2 * KV_HEADS * HD), jnp.bfloat16).at[target].set(packed)
    return (context, kv_cache)
```

```python
import functools
import math

import jax
import jax.numpy as jnp
from jax import lax
from jax.experimental import pallas as pl
from jax.experimental.pallas import tpu as pltpu
from jax.sharding import PartitionSpec as P

HD = 128
BLOCK = 128
EPSILON = 1e-06
THETA = 1000000.0
CORES = 2
VMEM_LIMIT = 64 * 1024 * 1024 - 128 * 1024
MESH = pl.DeviceIdType.MESH


def rope(x, cos2, sin2):
    return x * cos2 + pltpu.roll(x, HD // 2, 1) * sin2


def project_kernel(
    sizes,
    h_ref,
    gain_ref,
    wq_ref,
    wk_ref,
    wv_ref,
    cos_ref,
    sin_ref,
    own_ref,
    q_out,
    kv_out,
    own_out,
    hid,
    normed,
    wqf,
    wkf,
    wvf,
    kvf,
    ownf,
    local_sem,
    h_send,
    h_recv,
    sib_send,
    sib_recv,
    y_send,
    y_recv,
    x_send,
    x_recv,
    ys_send,
    ys_recv,
    xs_send,
    xs_recv,
    kv_send,
    kv_recv,
    o_send,
    o_recv,
):
    n_groups, n_dev, n_tp, q_chunks, pieces = sizes
    g = lax.axis_index("groups")
    d = lax.axis_index("dev")
    t = lax.axis_index("tp")
    ny = n_dev // CORES
    y = d // CORES
    core = d % CORES
    sib = y * CORES + (CORES - 1 - core)
    right, left = (t + 1) % n_tp, (t + n_tp - 1) % n_tp
    tok, feat = h_ref.shape
    sends = []

    def remote(src, dst, ssem, rsem, where):
        return pltpu.make_async_remote_copy(
            src_ref=src, dst_ref=dst, send_sem=ssem, recv_sem=rsem,
            device_id=where, device_id_type=MESH,
        )

    def send(src, dst, ssem, rsem, where):
        copy = remote(src, dst, ssem, rsem, where)
        copy.start()
        sends.append(copy)

    def landed(region, ssem, rsem, where):
        remote(region, region, ssem, rsem, where).wait_recv()

    barrier = pltpu.get_barrier_semaphore()
    count = 0
    for o in range(1, n_dev):
        pl.semaphore_signal(
            barrier, inc=1, device_id={"dev": (d + o) % n_dev}, device_id_type=MESH)
        count += 1
    for o in range(1, n_groups):
        pl.semaphore_signal(
            barrier, inc=1, device_id={"groups": (g + o) % n_groups}, device_id_type=MESH)
        count += 1
    for nb in (left, right):
        pl.semaphore_signal(barrier, inc=1, device_id={"tp": nb}, device_id_type=MESH)
        count += 1
    pl.semaphore_wait(barrier, count)

    own_w = (wk_ref, wv_ref, wq_ref)
    full_w = (wkf, wvf, wqf)
    chunks = [(0, 0, 0), (1, 0, 1)] + [(2, c, 2 + c) for c in range(q_chunks)]
    n_chunks = (1, 1, q_chunks)

    def own_part(a, c):
        rows = own_w[a].shape[0]
        size = rows // n_groups // n_chunks[a]
        first = pl.multiple_of(g * (rows // n_groups) + c * size, size)
        return own_w[a].at[pl.ds(first, size)]

    def full_part(a, c, dev, group):
        rows = own_w[a].shape[0]
        size = rows // n_groups // n_chunks[a]
        first = pl.multiple_of(dev * rows + group * (rows // n_groups) + c * size, size)
        return full_w[a].at[pl.ds(first, size)]

    def full_rows(a, dev):
        rows = own_w[a].shape[0]
        return full_w[a].at[pl.ds(pl.multiple_of(dev * rows, rows), rows)]

    prow = tok // pieces
    half = pieces // 2

    def hid_piece(block, p):
        first = pl.multiple_of(block * feat, 128)
        return hid.at[pl.ds(p * prow, prow), pl.ds(first, feat)]

    def own_piece(p):
        return h_ref.at[pl.ds(p * prow, prow)]

    def hops(direction, p):
        far = p < half if direction == 0 else p >= half
        return n_tp // 2 if far else n_tp // 2 - 1

    order = (
        list(range(pieces)),
        list(range(half, pieces)) + list(range(half)),
    )
    nbr = (right, left)

    def source(direction, s):
        return (t - s + n_tp) % n_tp if direction == 0 else (t + s) % n_tp

    for a, c, k in chunks[:2]:
        for oy in range(1, ny):
            peer = ((y + oy) % ny) * CORES + core
            send(own_part(a, c), full_part(a, c, d, g), y_send.at[oy - 1, k],
                 y_recv.at[oy - 1, k], {"dev": peer})
    for i in range(pieces):
        for direction in range(2):
            p = order[direction][i]
            if hops(direction, p) >= 1:
                send(own_piece(p), hid_piece(t, p), h_send.at[direction, 0, p],
                     h_recv.at[direction, 0, p], {"tp": nbr[direction]})
    for a, c, k in chunks[2:]:
        for oy in range(1, ny):
            peer = ((y + oy) % ny) * CORES + core
            send(own_part(a, c), full_part(a, c, d, g), y_send.at[oy - 1, k],
                 y_recv.at[oy - 1, k], {"dev": peer})
    for a in range(3):
        send(own_w[a], full_rows(a, d), sib_send.at[a], sib_recv.at[a], {"dev": sib})
    for o in range(1, n_dev):
        send(own_ref, ownf.at[d], o_send.at[o - 1], o_recv.at[o - 1], {"dev": (d + o) % n_dev})
    locals_ = []
    for a in range(3):
        locals_.append(pltpu.make_async_copy(own_w[a], full_rows(a, d), local_sem.at[a]))
    locals_.append(pltpu.make_async_copy(
        h_ref, hid.at[:, pl.ds(pl.multiple_of(t * feat, 128), feat)], local_sem.at[3]))
    locals_.append(pltpu.make_async_copy(own_ref, ownf.at[d], local_sem.at[4]))
    for copy in locals_:
        copy.start()

    def y_step(a, c, k):
        for oy in range(1, ny):
            dev = ((y - oy + ny) % ny) * CORES + core
            part = full_part(a, c, dev, g)
            landed(part, y_send.at[oy - 1, k], y_recv.at[oy - 1, k], {"dev": dev})
            for og in range(1, n_groups):
                send(part, part, x_send.at[oy - 1, og - 1, k], x_recv.at[oy - 1, og - 1, k],
                     {"groups": (g + og) % n_groups})
            send(part, part, ys_send.at[oy - 1, k], ys_recv.at[oy - 1, k], {"dev": sib})

    def x_step(a, c, k):
        for oy in range(1, ny):
            dev = ((y - oy + ny) % ny) * CORES + core
            for og in range(1, n_groups):
                group = (g - og + n_groups) % n_groups
                part = full_part(a, c, dev, group)
                landed(part, x_send.at[oy - 1, og - 1, k], x_recv.at[oy - 1, og - 1, k],
                       {"groups": group})
                send(part, part, xs_send.at[oy - 1, og - 1, k], xs_recv.at[oy - 1, og - 1, k],
                     {"dev": sib})

    def sib_done(a, c, k):
        for oy in range(1, ny):
            dev = ((y - oy + ny) % ny) * CORES + (CORES - 1 - core)
            part = full_part(a, c, dev, g)
            landed(part, ys_send.at[oy - 1, k], ys_recv.at[oy - 1, k], {"dev": sib})
            for og in range(1, n_groups):
                part = full_part(a, c, dev, (g - og + n_groups) % n_groups)
                landed(part, xs_send.at[oy - 1, og - 1, k], xs_recv.at[oy - 1, og - 1, k],
                       {"dev": sib})

    def h_step(s):
        for i in range(pieces):
            for direction in range(2):
                p = order[direction][i]
                if hops(direction, p) >= s + 1:
                    block = hid_piece(source(direction, s), p)
                    landed(block, h_send.at[direction, s - 1, p],
                           h_recv.at[direction, s - 1, p], {"tp": nbr[1 - direction]})
                    send(block, block, h_send.at[direction, s, p],
                         h_recv.at[direction, s, p], {"tp": nbr[direction]})

    y_step(*chunks[0])
    y_step(*chunks[1])
    for s in range(1, n_tp // 2):
        h_step(s)
    for i in range(2, len(chunks)):
        y_step(*chunks[i])
        x_step(*chunks[i - 2])
    for i in range(pieces):
        for direction in range(2):
            p = order[direction][i]
            s = hops(direction, p)
            if s >= 1:
                landed(hid_piece(source(direction, s), p), h_send.at[direction, s - 1, p],
                       h_recv.at[direction, s - 1, p], {"tp": nbr[1 - direction]})
    for copy in locals_:
        copy.wait()

    def norm_rows(i, _):
        rows = pl.ds(pl.multiple_of(i * 16, 16), 16)
        x = hid[rows, :].astype(jnp.float32)
        square = jnp.sum(x * x, axis=1, keepdims=True) * (1.0 / (feat * n_tp))
        normed[rows, :] = (x * lax.rsqrt(square + EPSILON) * gain_ref[...]).astype(jnp.bfloat16)
        return 0

    lax.fori_loop(0, tok // 16, norm_rows, 0)

    kv_width = wk_ref.shape[1]
    mine = pl.ds(pl.multiple_of(d * tok, tok), tok)
    for a in (0, 1):
        landed(full_rows(a, sib), sib_send.at[a], sib_recv.at[a], {"dev": sib})
        sib_done(*chunks[a])
        proj = jnp.dot(normed[...], full_w[a][...], preferred_element_type=jnp.float32)
        for head in range(kv_width // HD):
            part = proj[:, head * HD:(head + 1) * HD]
            if a == 0:
                part = rope(part, cos_ref[...], sin_ref[...])
            kvf[mine, (2 * head + a) * HD:(2 * head + a + 1) * HD] = part.astype(jnp.bfloat16)
    for i in range(len(chunks) - 2, len(chunks)):
        x_step(*chunks[i])
    send(kvf.at[mine], kvf.at[mine], kv_send.at[0, 0], kv_recv.at[0, 0], {"dev": sib})
    for oy in range(1, ny):
        peer = ((y + oy) % ny) * CORES + core
        send(kvf.at[mine], kvf.at[mine], kv_send.at[0, oy], kv_recv.at[0, oy], {"dev": peer})
    landed(full_rows(2, sib), sib_send.at[2], sib_recv.at[2], {"dev": sib})
    for i in range(2, len(chunks)):
        sib_done(*chunks[i])

    q_width = wq_ref.shape[1]
    tile = 256 if q_width % 256 == 0 else HD

    def q_tile(i, _):
        columns = pl.ds(pl.multiple_of(i * tile, tile), tile)
        proj = jnp.dot(normed[...], wqf[:, columns], preferred_element_type=jnp.float32)
        parts = [
            rope(proj[:, j * HD:(j + 1) * HD], cos_ref[...], sin_ref[...]).astype(jnp.bfloat16)
            for j in range(tile // HD)
        ]
        q_out[:, columns] = parts[0] if len(parts) == 1 else jnp.concatenate(parts, axis=1)
        return 0

    lax.fori_loop(0, q_width // tile, q_tile, 0)

    def kv_rows(dev):
        return kvf.at[pl.ds(pl.multiple_of(dev * tok, tok), tok)]

    for oy in range(1, ny):
        dev = ((y - oy + ny) % ny) * CORES + core
        part = kv_rows(dev)
        landed(part, kv_send.at[0, oy], kv_recv.at[0, oy], {"dev": dev})
        send(part, part, kv_send.at[1, oy], kv_recv.at[1, oy], {"dev": sib})
    landed(kv_rows(sib), kv_send.at[0, 0], kv_recv.at[0, 0], {"dev": sib})
    for oy in range(1, ny):
        dev = ((y - oy + ny) % ny) * CORES + (CORES - 1 - core)
        landed(kv_rows(dev), kv_send.at[1, oy], kv_recv.at[1, oy], {"dev": sib})
    for o in range(1, n_dev):
        dev = (d - o + n_dev) % n_dev
        landed(ownf.at[dev], o_send.at[o - 1], o_recv.at[o - 1], {"dev": dev})
    for copy in sends:
        copy.wait_send()
    kv_out[...] = kvf[...]
    own_out[...] = ownf[...]


def attend_kernel(
    blk_dev, group_size, prompt_ref, owner_ref, slot_ref, dev_ref, q_ref, kv_ref, ctx_ref,
    cache_ref
):
    tok, q_width = q_ref.shape
    heads = q_width // HD
    kv_heads = heads // group_size
    d = dev_ref[0]
    n_prompts = prompt_ref.shape[0]
    scale = 1.0 / math.sqrt(HD)

    cache_ref[...] = jnp.zeros_like(cache_ref)

    def place(b, rank):
        hit = owner_ref[b] == d
        @pl.when(hit)
        def _():
            cache_ref[slot_ref[rank]] = kv_ref[pl.ds(pl.multiple_of(b * BLOCK, BLOCK), BLOCK), :]
        return rank + hit.astype(jnp.int32)

    lax.fori_loop(0, owner_ref.shape[0], place, jnp.int32(0))

    stacked = group_size * BLOCK
    row = lax.broadcasted_iota(jnp.int32, (group_size, BLOCK, BLOCK), 1).reshape(stacked, BLOCK)
    col = lax.broadcasted_iota(jnp.int32, (group_size, BLOCK, BLOCK), 2).reshape(stacked, BLOCK)
    causal = col <= row

    def q_block(b, _):
        block = d * blk_dev + b
        first = jnp.int32(0)
        total = jnp.int32(0)
        for p in range(n_prompts):
            first = jnp.where(total <= block, total, first)
            total = total + prompt_ref[p]
        rows = pl.ds(pl.multiple_of(b * BLOCK, BLOCK), BLOCK)
        for kh in range(kv_heads):
            q = jnp.concatenate(
                [
                    q_ref[rows, (kh * group_size + j) * HD:(kh * group_size + j + 1) * HD]
                    for j in range(group_size)
                ],
                axis=0,
            )

            def scores_of(j):
                at = pl.ds(pl.multiple_of(j * BLOCK, BLOCK), BLOCK)
                keys = kv_ref[at, 2 * kh * HD:(2 * kh + 1) * HD]
                values = kv_ref[at, (2 * kh + 1) * HD:(2 * kh + 2) * HD]
                s = lax.dot_general(
                    q, keys, (((1,), (1,)), ((), ())), preferred_element_type=jnp.float32
                ) * scale
                return s, values

            s, values = scores_of(block)
            s = jnp.where(causal, s, -1e30)
            m = jnp.max(s, axis=1, keepdims=True)
            w = jnp.where(causal, jnp.exp(s - m), 0.0)
            l = jnp.sum(w, axis=1, keepdims=True)
            acc = jnp.dot(w.astype(jnp.bfloat16), values, preferred_element_type=jnp.float32)

            def step(j, carry):
                m, l, acc = carry
                s, values = scores_of(j)
                m2 = jnp.maximum(m, jnp.max(s, axis=1, keepdims=True))
                w = jnp.exp(s - m2)
                decay = jnp.exp(m - m2)
                l = l * decay + jnp.sum(w, axis=1, keepdims=True)
                acc = acc * decay + jnp.dot(
                    w.astype(jnp.bfloat16), values, preferred_element_type=jnp.float32
                )
                return m2, l, acc

            m, l, acc = lax.fori_loop(first, block, step, (m, l, acc))
            out = (acc / l).astype(jnp.bfloat16)
            for j in range(group_size):
                ctx_ref[rows, (kh * group_size + j) * HD:(kh * group_size + j + 1) * HD] = (
                    out[j * BLOCK:(j + 1) * BLOCK]
                )
        return 0

    lax.fori_loop(0, blk_dev, q_block, 0)


def on_device(
    hidden_states, norm_gain, w_query, w_key, w_value, prompt_blocks, owner_map, slot_table
):
    n_groups, n_dev, n_tp = (lax.axis_size(a) for a in ("groups", "dev", "tp"))
    device = lax.axis_index("dev")
    tok, feat = hidden_states.shape
    width = feat * n_tp
    q_width, kv_width = w_query.shape[1], w_key.shape[1]
    ny = n_dev // CORES
    blk_dev = owner_map.shape[0]

    token_rows = device * tok + jnp.arange(tok, dtype=jnp.int32)
    starts = jnp.sum(
        jnp.where(
            jnp.arange(prompt_blocks.shape[0])[None, :] < jnp.arange(prompt_blocks.shape[0])[:, None],
            prompt_blocks[None, :], 0), axis=1) * BLOCK
    start_of = jnp.max(
        jnp.where(token_rows[:, None] >= starts[None, :], starts[None, :], 0), axis=1)
    offsets = (token_rows - start_of).astype(jnp.float32)
    freq = jnp.arange(HD // 2, dtype=jnp.float32)
    inverse = jnp.exp(freq * (-2.0 * math.log(THETA) / HD))
    inverse = jnp.concatenate([inverse, inverse])
    sign = jnp.where(jnp.arange(HD) < HD // 2, -1.0, 1.0)
    angles = offsets[:, None] * inverse[None, :]
    cos2, sin2 = jnp.cos(angles), jnp.sin(angles) * sign[None, :]

    own = jnp.pad(owner_map[None, :], ((0, 7), (0, 128 - blk_dev)))
    q_chunks = 4 if ny == 2 else 1
    n_chunks = 2 + q_chunks
    pieces = 8 if n_tp == 4 else 2
    dma = pltpu.SemaphoreType.DMA
    far = max(ny - 1, 1)
    og = max(n_groups - 1, 1)
    hop = max(n_tp // 2, 1)
    vmem = pl.BlockSpec(memory_space=pltpu.VMEM)
    flops = 2 * tok * width * (q_width + 2 * kv_width)
    queries, kv_all, owners = pl.pallas_call(
        functools.partial(project_kernel, (n_groups, n_dev, n_tp, q_chunks, pieces)),
        out_shape=(
            jax.ShapeDtypeStruct((tok, q_width), jnp.bfloat16),
            jax.ShapeDtypeStruct((n_dev * tok, 2 * kv_width), jnp.bfloat16),
            jax.ShapeDtypeStruct((n_dev, 8, 128), jnp.int32),
        ),
        in_specs=[vmem] * 8,
        out_specs=(vmem, vmem, vmem),
        scratch_shapes=[
            pltpu.VMEM((tok, width), jnp.bfloat16),
            pltpu.VMEM((tok, width), jnp.bfloat16),
            pltpu.VMEM((width, q_width), jnp.bfloat16),
            pltpu.VMEM((width, kv_width), jnp.bfloat16),
            pltpu.VMEM((width, kv_width), jnp.bfloat16),
            pltpu.VMEM((n_dev * tok, 2 * kv_width), jnp.bfloat16),
            pltpu.VMEM((n_dev, 8, 128), jnp.int32),
            dma((5,)),
            dma((2, hop, pieces)), dma((2, hop, pieces)),
            dma((3,)), dma((3,)),
            dma((far, n_chunks)), dma((far, n_chunks)),
            dma((far, og, n_chunks)), dma((far, og, n_chunks)),
            dma((far, n_chunks)), dma((far, n_chunks)),
            dma((far, og, n_chunks)), dma((far, og, n_chunks)),
            dma((2, ny)), dma((2, ny)),
            dma((n_dev - 1,)), dma((n_dev - 1,)),
        ],
        cost_estimate=pl.CostEstimate(
            flops=flops, bytes_accessed=2 * width * (q_width + 2 * kv_width + tok),
            transcendentals=0),
        compiler_params=pltpu.CompilerParams(
            collective_id=0, has_side_effects=True, vmem_limit_bytes=VMEM_LIMIT),
    )(
        hidden_states, norm_gain.astype(jnp.float32)[None, :], w_query, w_key, w_value, cos2, sin2,
        own,
    )

    smem = pl.BlockSpec(memory_space=pltpu.SMEM)
    slots = slot_table.shape[1]
    return pl.pallas_call(
        functools.partial(attend_kernel, blk_dev, q_width // kv_width),
        out_shape=(
            jax.ShapeDtypeStruct((tok, q_width), jnp.bfloat16),
            jax.ShapeDtypeStruct((slots, BLOCK, 2 * kv_width), jnp.bfloat16),
        ),
        in_specs=[smem] * 4 + [vmem] * 2,
        out_specs=(vmem, vmem),
        compiler_params=pltpu.CompilerParams(vmem_limit_bytes=VMEM_LIMIT),
    )(
        prompt_blocks, owners[:, 0, :blk_dev].reshape(-1), slot_table[0],
        device.astype(jnp.int32)[None], queries, kv_all,
    )


def solution(mesh):
    in_specs = (
        P(("groups", "dev"), "tp"),
        P(),
        P("dev", "tp"),
        P("dev", "tp"),
        P("dev", "tp"),
        P("groups"),
        P(("groups", "dev")),
        P(("groups", "dev"), None),
    )
    out_specs = (P(("groups", "dev"), "tp"), P(("groups", "dev"), None, "tp"))
    return jax.shard_map(
        on_device, mesh=mesh, in_specs=in_specs, out_specs=out_specs, check_vma=False
    )
```

```python
import functools
import math

import jax
import jax.numpy as jnp
from jax import lax
from jax.experimental import pallas as pl
from jax.experimental.pallas import tpu as pltpu
from jax.sharding import PartitionSpec as P

HD = 128
BLOCK = 128
EPSILON = 1e-06
THETA = 1000000.0
CORES = 2
VMEM_LIMIT = 64 * 1024 * 1024 - 128 * 1024
MESH = pl.DeviceIdType.MESH


def rope(x, cos2, sin2):
    return x * cos2 + pltpu.roll(x, HD // 2, 1) * sin2


def project_kernel(
    sizes,
    h_ref,
    gain_ref,
    wq_ref,
    wk_ref,
    wv_ref,
    cos_ref,
    sin_ref,
    own_ref,
    q_out,
    kv_out,
    own_out,
    hid,
    scaled,
    squares,
    q_acc,
    kv_acc,
    wqf,
    wkf,
    wvf,
    kvf,
    ownf,
    local_sem,
    h_send,
    h_recv,
    sib_send,
    sib_recv,
    y_send,
    y_recv,
    x_send,
    x_recv,
    ys_send,
    ys_recv,
    xs_send,
    xs_recv,
    kv_send,
    kv_recv,
    o_send,
    o_recv,
):
    n_groups, n_dev, n_tp, q_chunks, pieces = sizes
    g = lax.axis_index("groups")
    d = lax.axis_index("dev")
    t = lax.axis_index("tp")
    ny = n_dev // CORES
    y = d // CORES
    core = d % CORES
    sib = y * CORES + (CORES - 1 - core)
    right, left = (t + 1) % n_tp, (t + n_tp - 1) % n_tp
    tok, feat = h_ref.shape
    sends = []

    def remote(src, dst, ssem, rsem, where):
        return pltpu.make_async_remote_copy(
            src_ref=src, dst_ref=dst, send_sem=ssem, recv_sem=rsem,
            device_id=where, device_id_type=MESH,
        )

    def send(src, dst, ssem, rsem, where):
        copy = remote(src, dst, ssem, rsem, where)
        copy.start()
        sends.append(copy)

    def landed(region, ssem, rsem, where):
        remote(region, region, ssem, rsem, where).wait_recv()

    barrier = pltpu.get_barrier_semaphore()
    count = 0
    for o in range(1, n_dev):
        pl.semaphore_signal(
            barrier, inc=1, device_id={"dev": (d + o) % n_dev}, device_id_type=MESH)
        count += 1
    for o in range(1, n_groups):
        pl.semaphore_signal(
            barrier, inc=1, device_id={"groups": (g + o) % n_groups}, device_id_type=MESH)
        count += 1
    for nb in (left, right):
        pl.semaphore_signal(barrier, inc=1, device_id={"tp": nb}, device_id_type=MESH)
        count += 1
    pl.semaphore_wait(barrier, count)

    own_w = (wk_ref, wv_ref, wq_ref)
    full_w = (wkf, wvf, wqf)
    chunks = [(0, 0, 0), (1, 0, 1)] + [(2, c, 2 + c) for c in range(q_chunks)]
    n_chunks = (1, 1, q_chunks)

    def own_part(a, c):
        rows = own_w[a].shape[0]
        size = rows // n_groups // n_chunks[a]
        first = pl.multiple_of(g * (rows // n_groups) + c * size, size)
        return own_w[a].at[pl.ds(first, size)]

    def full_part(a, c, dev, group):
        rows = own_w[a].shape[0]
        size = rows // n_groups // n_chunks[a]
        first = pl.multiple_of(dev * rows + group * (rows // n_groups) + c * size, size)
        return full_w[a].at[pl.ds(first, size)]

    def full_rows(a, dev):
        rows = own_w[a].shape[0]
        return full_w[a].at[pl.ds(pl.multiple_of(dev * rows, rows), rows)]

    prow = tok // pieces
    half = pieces // 2

    def hid_piece(block, p):
        first = pl.multiple_of(block * feat, 128)
        return hid.at[pl.ds(p * prow, prow), pl.ds(first, feat)]

    def own_piece(p):
        return h_ref.at[pl.ds(p * prow, prow)]

    def hops(direction, p):
        far = p < half if direction == 0 else p >= half
        return n_tp // 2 if far else n_tp // 2 - 1

    order = (
        list(range(pieces)),
        list(range(half, pieces)) + list(range(half)),
    )
    nbr = (right, left)

    def source(direction, s):
        return (t - s + n_tp) % n_tp if direction == 0 else (t + s) % n_tp

    for a, c, k in chunks[:2]:
        for oy in range(1, ny):
            peer = ((y + oy) % ny) * CORES + core
            send(own_part(a, c), full_part(a, c, d, g), y_send.at[oy - 1, k],
                 y_recv.at[oy - 1, k], {"dev": peer})
    for i in range(pieces):
        for direction in range(2):
            p = order[direction][i]
            if hops(direction, p) >= 1:
                send(own_piece(p), hid_piece(t, p), h_send.at[direction, 0, p],
                     h_recv.at[direction, 0, p], {"tp": nbr[direction]})
    for a, c, k in chunks[2:]:
        for oy in range(1, ny):
            peer = ((y + oy) % ny) * CORES + core
            send(own_part(a, c), full_part(a, c, d, g), y_send.at[oy - 1, k],
                 y_recv.at[oy - 1, k], {"dev": peer})
    for a in range(3):
        send(own_w[a], full_rows(a, d), sib_send.at[a], sib_recv.at[a], {"dev": sib})
    for o in range(1, n_dev):
        send(own_ref, ownf.at[d], o_send.at[o - 1], o_recv.at[o - 1], {"dev": (d + o) % n_dev})
    locals_ = []
    for a in range(3):
        locals_.append(pltpu.make_async_copy(own_w[a], full_rows(a, d), local_sem.at[a]))
    locals_.append(pltpu.make_async_copy(
        h_ref, hid.at[:, pl.ds(pl.multiple_of(t * feat, 128), feat)], local_sem.at[3]))
    locals_.append(pltpu.make_async_copy(own_ref, ownf.at[d], local_sem.at[4]))
    for copy in locals_:
        copy.start()

    def y_step(a, c, k):
        for oy in range(1, ny):
            dev = ((y - oy + ny) % ny) * CORES + core
            part = full_part(a, c, dev, g)
            landed(part, y_send.at[oy - 1, k], y_recv.at[oy - 1, k], {"dev": dev})
            for og in range(1, n_groups):
                send(part, part, x_send.at[oy - 1, og - 1, k], x_recv.at[oy - 1, og - 1, k],
                     {"groups": (g + og) % n_groups})
            send(part, part, ys_send.at[oy - 1, k], ys_recv.at[oy - 1, k], {"dev": sib})

    def x_step(a, c, k):
        for oy in range(1, ny):
            dev = ((y - oy + ny) % ny) * CORES + core
            for og in range(1, n_groups):
                group = (g - og + n_groups) % n_groups
                part = full_part(a, c, dev, group)
                landed(part, x_send.at[oy - 1, og - 1, k], x_recv.at[oy - 1, og - 1, k],
                       {"groups": group})
                send(part, part, xs_send.at[oy - 1, og - 1, k], xs_recv.at[oy - 1, og - 1, k],
                     {"dev": sib})

    def sib_done(a, c, k):
        for oy in range(1, ny):
            dev = ((y - oy + ny) % ny) * CORES + (CORES - 1 - core)
            part = full_part(a, c, dev, g)
            landed(part, ys_send.at[oy - 1, k], ys_recv.at[oy - 1, k], {"dev": sib})
            for og in range(1, n_groups):
                part = full_part(a, c, dev, (g - og + n_groups) % n_groups)
                landed(part, xs_send.at[oy - 1, og - 1, k], xs_recv.at[oy - 1, og - 1, k],
                       {"dev": sib})

    def h_relay(s, direction, p):
        block = hid_piece(source(direction, s), p)
        landed(block, h_send.at[direction, s - 1, p],
               h_recv.at[direction, s - 1, p], {"tp": nbr[1 - direction]})
        send(block, block, h_send.at[direction, s, p],
             h_recv.at[direction, s, p], {"tp": nbr[direction]})

    def h_last(s, direction, p):
        landed(hid_piece(source(direction, s), p), h_send.at[direction, s - 1, p],
               h_recv.at[direction, s - 1, p], {"tp": nbr[1 - direction]})

    relays, lasts = [], []
    reach = n_tp // 2
    for s in range(1, reach + 1):
        for i in range(pieces):
            for direction in range(2):
                p = order[direction][i]
                if hops(direction, p) >= s + 1:
                    relays.append((s, direction, p))
                elif hops(direction, p) == s:
                    lasts.append((s, direction, p))

    per = -(-len(relays) // q_chunks)
    y_step(*chunks[0])
    y_step(*chunks[1])
    for i in range(2, len(chunks)):
        y_step(*chunks[i])
        x_step(*chunks[i - 2])
        for relay in relays[(i - 2) * per:(i - 1) * per]:
            h_relay(*relay)
    for i in range(len(chunks) - 2, len(chunks)):
        x_step(*chunks[i])
    for copy in locals_:
        copy.wait()

    step_rows = 16

    def scale_rows(block, first, count, fresh):
        columns = pl.ds(pl.multiple_of(block * feat, 128), feat)

        def body(i, _):
            rows = pl.ds(pl.multiple_of(first + i * step_rows, step_rows), step_rows)
            x = hid[rows, columns].astype(jnp.float32)
            total = jnp.broadcast_to(jnp.sum(x * x, axis=1, keepdims=True), (step_rows, HD))
            squares[rows, :] = total if fresh else squares[rows, :] + total
            scaled[rows, columns] = (x * gain_ref[:, columns]).astype(jnp.bfloat16)
            return 0

        lax.fori_loop(0, count // step_rows, body, 0)

    def block_dot(block, w, columns):
        k = pl.ds(pl.multiple_of(block * feat, 128), feat)
        return jnp.dot(scaled[:, k], w[k, columns], preferred_element_type=jnp.float32)

    scale_rows(t, 0, tok, True)
    near = [t]
    for s in range(1, reach):
        for last in lasts:
            if last[0] == s:
                h_last(*last)
        for direction in range(2):
            block = source(direction, s)
            near.append(block)
            scale_rows(block, 0, tok, False)

    kv_width = wk_ref.shape[1]
    mine = pl.ds(pl.multiple_of(d * tok, tok), tok)
    all_kv = pl.ds(0, kv_width)
    for a in range(3):
        landed(full_rows(a, sib), sib_send.at[a], sib_recv.at[a], {"dev": sib})
    for chunk in chunks:
        sib_done(*chunk)

    q_width = wq_ref.shape[1]
    tile = 256 if q_width % 256 == 0 else HD

    def near_dot(w, columns):
        total = block_dot(near[0], w, columns)
        for block in near[1:]:
            total = total + block_dot(block, w, columns)
        return total

    for a in (0, 1):
        kv_acc[:, a * kv_width:(a + 1) * kv_width] = near_dot(full_w[a], all_kv)

    def q_near(i, _):
        columns = pl.ds(pl.multiple_of(i * tile, tile), tile)
        q_acc[:, columns] = near_dot(wqf, columns)
        return 0

    lax.fori_loop(0, q_width // tile, q_near, 0)

    far_block = source(0, reach)
    for last in lasts:
        if last[0] == reach:
            h_last(*last)
            scale_rows(far_block, last[2] * prow, prow, False)
    squares[...] = lax.rsqrt(squares[...] * (1.0 / (feat * n_tp)) + EPSILON)

    for a in (0, 1):
        proj = kv_acc[:, a * kv_width:(a + 1) * kv_width] + block_dot(far_block, full_w[a], all_kv)
        for head in range(kv_width // HD):
            part = proj[:, head * HD:(head + 1) * HD] * squares[...]
            if a == 0:
                part = rope(part, cos_ref[...], sin_ref[...])
            kvf[mine, (2 * head + a) * HD:(2 * head + a + 1) * HD] = part.astype(jnp.bfloat16)
    for oy in range(1, ny):
        peer = ((y + oy) % ny) * CORES + core
        send(kvf.at[mine], kvf.at[mine], kv_send.at[0, oy], kv_recv.at[0, oy], {"dev": peer})
    send(kvf.at[mine], kvf.at[mine], kv_send.at[0, 0], kv_recv.at[0, 0], {"dev": sib})

    def q_tile(i, _):
        columns = pl.ds(pl.multiple_of(i * tile, tile), tile)
        proj = q_acc[:, columns] + block_dot(far_block, wqf, columns)
        parts = [
            rope(
                proj[:, j * HD:(j + 1) * HD] * squares[...], cos_ref[...], sin_ref[...]
            ).astype(jnp.bfloat16)
            for j in range(tile // HD)
        ]
        q_out[:, columns] = parts[0] if len(parts) == 1 else jnp.concatenate(parts, axis=1)
        return 0

    lax.fori_loop(0, q_width // tile, q_tile, 0)

    def kv_rows(dev):
        return kvf.at[pl.ds(pl.multiple_of(dev * tok, tok), tok)]

    for oy in range(1, ny):
        dev = ((y - oy + ny) % ny) * CORES + core
        part = kv_rows(dev)
        landed(part, kv_send.at[0, oy], kv_recv.at[0, oy], {"dev": dev})
        send(part, part, kv_send.at[1, oy], kv_recv.at[1, oy], {"dev": sib})
    landed(kv_rows(sib), kv_send.at[0, 0], kv_recv.at[0, 0], {"dev": sib})
    for oy in range(1, ny):
        dev = ((y - oy + ny) % ny) * CORES + (CORES - 1 - core)
        landed(kv_rows(dev), kv_send.at[1, oy], kv_recv.at[1, oy], {"dev": sib})
    for o in range(1, n_dev):
        dev = (d - o + n_dev) % n_dev
        landed(ownf.at[dev], o_send.at[o - 1], o_recv.at[o - 1], {"dev": dev})
    for copy in sends:
        copy.wait_send()
    kv_out[...] = kvf[...]
    own_out[...] = ownf[...]


def attend_kernel(
    blk_dev, group_size, prompt_ref, owner_ref, slot_ref, dev_ref, q_ref, kv_ref, ctx_ref,
    cache_ref
):
    tok, q_width = q_ref.shape
    heads = q_width // HD
    kv_heads = heads // group_size
    d = dev_ref[0]
    n_prompts = prompt_ref.shape[0]
    scale = 1.0 / math.sqrt(HD)

    cache_ref[...] = jnp.zeros_like(cache_ref)

    def place(b, rank):
        hit = owner_ref[b] == d
        @pl.when(hit)
        def _():
            cache_ref[slot_ref[rank]] = kv_ref[pl.ds(pl.multiple_of(b * BLOCK, BLOCK), BLOCK), :]
        return rank + hit.astype(jnp.int32)

    lax.fori_loop(0, owner_ref.shape[0], place, jnp.int32(0))

    stacked = group_size * BLOCK
    row = lax.broadcasted_iota(jnp.int32, (group_size, BLOCK, BLOCK), 1).reshape(stacked, BLOCK)
    col = lax.broadcasted_iota(jnp.int32, (group_size, BLOCK, BLOCK), 2).reshape(stacked, BLOCK)
    causal = col <= row

    def q_block(b, _):
        block = d * blk_dev + b
        first = jnp.int32(0)
        total = jnp.int32(0)
        for p in range(n_prompts):
            first = jnp.where(total <= block, total, first)
            total = total + prompt_ref[p]
        rows = pl.ds(pl.multiple_of(b * BLOCK, BLOCK), BLOCK)
        q_heads = [
            jnp.concatenate(
                [
                    q_ref[rows, (kh * group_size + j) * HD:(kh * group_size + j + 1) * HD]
                    for j in range(group_size)
                ],
                axis=0,
            )
            for kh in range(kv_heads)
        ]

        def scores_of(j, kh):
            at = pl.ds(pl.multiple_of(j * BLOCK, BLOCK), BLOCK)
            keys = kv_ref[at, 2 * kh * HD:(2 * kh + 1) * HD]
            values = kv_ref[at, (2 * kh + 1) * HD:(2 * kh + 2) * HD]
            s = lax.dot_general(
                q_heads[kh], keys, (((1,), (1,)), ((), ())), preferred_element_type=jnp.float32
            ) * scale
            return s, values

        carry = []
        for kh in range(kv_heads):
            s, values = scores_of(block, kh)
            s = jnp.where(causal, s, -1e30)
            m = jnp.max(s, axis=1, keepdims=True)
            w = jnp.exp(s - m)
            l = jnp.sum(w, axis=1, keepdims=True)
            acc = jnp.dot(w.astype(jnp.bfloat16), values, preferred_element_type=jnp.float32)
            carry.append((m, l, acc))

        def step(j, carry):
            new = []
            for kh in range(kv_heads):
                m, l, acc = carry[kh]
                s, values = scores_of(j, kh)
                m2 = jnp.maximum(m, jnp.max(s, axis=1, keepdims=True))
                w = jnp.exp(s - m2)
                decay = jnp.exp(m - m2)
                l = l * decay + jnp.sum(w, axis=1, keepdims=True)
                acc = acc * decay + jnp.dot(
                    w.astype(jnp.bfloat16), values, preferred_element_type=jnp.float32
                )
                new.append((m2, l, acc))
            return tuple(new)

        carry = lax.fori_loop(first, block, step, tuple(carry))
        for kh in range(kv_heads):
            m, l, acc = carry[kh]
            out = (acc / l).astype(jnp.bfloat16)
            for j in range(group_size):
                ctx_ref[rows, (kh * group_size + j) * HD:(kh * group_size + j + 1) * HD] = (
                    out[j * BLOCK:(j + 1) * BLOCK]
                )
        return 0

    lax.fori_loop(0, blk_dev, q_block, 0)


def on_device(
    hidden_states, norm_gain, w_query, w_key, w_value, prompt_blocks, owner_map, slot_table
):
    n_groups, n_dev, n_tp = (lax.axis_size(a) for a in ("groups", "dev", "tp"))
    device = lax.axis_index("dev")
    tok, feat = hidden_states.shape
    width = feat * n_tp
    q_width, kv_width = w_query.shape[1], w_key.shape[1]
    ny = n_dev // CORES
    blk_dev = owner_map.shape[0]

    token_rows = device * tok + jnp.arange(tok, dtype=jnp.int32)
    starts = jnp.sum(
        jnp.where(
            jnp.arange(prompt_blocks.shape[0])[None, :] < jnp.arange(prompt_blocks.shape[0])[:, None],
            prompt_blocks[None, :], 0), axis=1) * BLOCK
    start_of = jnp.max(
        jnp.where(token_rows[:, None] >= starts[None, :], starts[None, :], 0), axis=1)
    offsets = (token_rows - start_of).astype(jnp.float32)
    freq = jnp.arange(HD // 2, dtype=jnp.float32)
    inverse = jnp.exp(freq * (-2.0 * math.log(THETA) / HD))
    inverse = jnp.concatenate([inverse, inverse])
    sign = jnp.where(jnp.arange(HD) < HD // 2, -1.0, 1.0)
    angles = offsets[:, None] * inverse[None, :]
    cos2, sin2 = jnp.cos(angles), jnp.sin(angles) * sign[None, :]

    own = jnp.pad(owner_map[None, :], ((0, 7), (0, 128 - blk_dev)))
    q_chunks = 4 if ny == 2 else 1
    n_chunks = 2 + q_chunks
    pieces = 8 if n_tp == 4 else 2
    dma = pltpu.SemaphoreType.DMA
    far = max(ny - 1, 1)
    og = max(n_groups - 1, 1)
    hop = max(n_tp // 2, 1)
    vmem = pl.BlockSpec(memory_space=pltpu.VMEM)
    flops = 2 * tok * width * (q_width + 2 * kv_width)
    queries, kv_all, owners = pl.pallas_call(
        functools.partial(project_kernel, (n_groups, n_dev, n_tp, q_chunks, pieces)),
        out_shape=(
            jax.ShapeDtypeStruct((tok, q_width), jnp.bfloat16),
            jax.ShapeDtypeStruct((n_dev * tok, 2 * kv_width), jnp.bfloat16),
            jax.ShapeDtypeStruct((n_dev, 8, 128), jnp.int32),
        ),
        in_specs=[vmem] * 8,
        out_specs=(vmem, vmem, vmem),
        scratch_shapes=[
            pltpu.VMEM((tok, width), jnp.bfloat16),
            pltpu.VMEM((tok, width), jnp.bfloat16),
            pltpu.VMEM((tok, HD), jnp.float32),
            pltpu.VMEM((tok, q_width), jnp.float32),
            pltpu.VMEM((tok, 2 * kv_width), jnp.float32),
            pltpu.VMEM((width, q_width), jnp.bfloat16),
            pltpu.VMEM((width, kv_width), jnp.bfloat16),
            pltpu.VMEM((width, kv_width), jnp.bfloat16),
            pltpu.VMEM((n_dev * tok, 2 * kv_width), jnp.bfloat16),
            pltpu.VMEM((n_dev, 8, 128), jnp.int32),
            dma((5,)),
            dma((2, hop, pieces)), dma((2, hop, pieces)),
            dma((3,)), dma((3,)),
            dma((far, n_chunks)), dma((far, n_chunks)),
            dma((far, og, n_chunks)), dma((far, og, n_chunks)),
            dma((far, n_chunks)), dma((far, n_chunks)),
            dma((far, og, n_chunks)), dma((far, og, n_chunks)),
            dma((2, ny)), dma((2, ny)),
            dma((n_dev - 1,)), dma((n_dev - 1,)),
        ],
        cost_estimate=pl.CostEstimate(
            flops=flops, bytes_accessed=2 * width * (q_width + 2 * kv_width + tok),
            transcendentals=0),
        compiler_params=pltpu.CompilerParams(
            collective_id=0, has_side_effects=True, vmem_limit_bytes=VMEM_LIMIT),
    )(
        hidden_states, norm_gain.astype(jnp.float32)[None, :], w_query, w_key, w_value, cos2, sin2,
        own,
    )

    smem = pl.BlockSpec(memory_space=pltpu.SMEM)
    slots = slot_table.shape[1]
    return pl.pallas_call(
        functools.partial(attend_kernel, blk_dev, q_width // kv_width),
        out_shape=(
            jax.ShapeDtypeStruct((tok, q_width), jnp.bfloat16),
            jax.ShapeDtypeStruct((slots, BLOCK, 2 * kv_width), jnp.bfloat16),
        ),
        in_specs=[smem] * 4 + [vmem] * 2,
        out_specs=(vmem, vmem),
        compiler_params=pltpu.CompilerParams(vmem_limit_bytes=VMEM_LIMIT),
    )(
        prompt_blocks, owners[:, 0, :blk_dev].reshape(-1), slot_table[0],
        device.astype(jnp.int32)[None], queries, kv_all,
    )


def solution(mesh):
    in_specs = (
        P(("groups", "dev"), "tp"),
        P(),
        P("dev", "tp"),
        P("dev", "tp"),
        P("dev", "tp"),
        P("groups"),
        P(("groups", "dev")),
        P(("groups", "dev"), None),
    )
    out_specs = (P(("groups", "dev"), "tp"), P(("groups", "dev"), None, "tp"))
    return jax.shard_map(
        on_device, mesh=mesh, in_specs=in_specs, out_specs=out_specs, check_vma=False
    )
```
